16 devices in a mesh: dp: 1, sp: 16 (over x, y, z, core).
Axes of the slice: x: 2, y: 2, z: 2, core: 2. Of those that a mesh axis runs over, the one named last changes fastest.
Arguments:
- x: bfloat16 [4096, 4096], P(('dp', 'sp'))
- gain: bfloat16 [4096], replicated
- wq: bfloat16 [4096, 4096], replicated
- wk: bfloat16 [4096, 4096], replicated
- wv: bfloat16 [4096, 4096], replicated
- wo: bfloat16 [4096, 4096], replicated
Outputs:
- output: bfloat16 [4096, 4096], P(('dp', 'sp'))
All inputs are finite; a program needn't handle non-finite values.
Results may differ from the reference program's by a relative error of at most 0.012.
Values are sent between devices in bfloat16 or wider.
A program may use at most 2 GiB of HBM per device.

```python
import jax
import jax.numpy as jnp
from jax import lax

ROWS = 4096
D = 4096
HEADS = 32
KV_HEADS = 32
HEAD = 128
THETA = 10000


def setup_inputs(seed: int = 0, part: int = 0) -> dict:
    kx, kn, kq, kk, kv, ko = jax.random.split(jax.random.key(seed), 6)

    def weights(key, rows, columns):
        return jax.random.normal(key, (rows, columns), jnp.float32) * rows**-0.5

    drawn = {
        "x": jax.random.normal(jax.random.fold_in(kx, part), (ROWS, D), jnp.float32),
        "gain": 1 + 0.1 * jax.random.normal(kn, (D,), jnp.float32),
        "wq": 2 * weights(kq, D, HEADS * HEAD),
        "wk": 2 * weights(kk, D, KV_HEADS * HEAD),
        "wv": 4 * weights(kv, D, KV_HEADS * HEAD),
        "wo": weights(ko, HEADS * HEAD, D),
    }
    return {k: v.astype(jnp.bfloat16) for k, v in drawn.items()}


def normed(x, gain):
    wide = x.astype(jnp.float32)
    scale = lax.rsqrt(jnp.mean(wide * wide, -1, keepdims=True) + 1e-6)
    return (wide * scale * gain.astype(jnp.float32)).astype(jnp.bfloat16)


def turned(t, place, theta):
    half = t.shape[-1] // 2
    angle = place.astype(jnp.float32)[:, None] * theta ** (-jnp.arange(half, dtype=jnp.float32) / half)
    cos, sin = jnp.cos(angle)[:, None], jnp.sin(angle)[:, None]
    a, b = t[..., :half].astype(jnp.float32), t[..., half:].astype(jnp.float32)
    return jnp.concatenate([a * cos - b * sin, b * cos + a * sin], -1).astype(jnp.bfloat16)


def matmul(a, w):
    return jnp.dot(a, w, preferred_element_type=jnp.float32).astype(jnp.bfloat16)


def einsum(form, a, b):
    return jnp.einsum(form, a.astype(jnp.float32), b.astype(jnp.float32))


def attention(q, k, v):
    scores = einsum("tgsd,ugd->gstu", q, k) * q.shape[-1] ** -0.5
    token = jnp.arange(q.shape[0])
    scores = jnp.where(token[:, None] >= token, scores, -jnp.inf)
    weights = jax.nn.softmax(scores, -1).astype(jnp.bfloat16)
    return einsum("gstu,ugd->tgsd", weights, v).astype(jnp.bfloat16)


def reference(x, gain, wq, wk, wv, wo):
    a, place = normed(x, gain), jnp.arange(ROWS)
    q = turned(matmul(a, wq).reshape(ROWS, HEADS, HEAD), place, THETA).reshape(ROWS, KV_HEADS, -1, HEAD)
    k = turned(matmul(a, wk).reshape(ROWS, KV_HEADS, HEAD), place, THETA)
    v = matmul(a, wv).reshape(ROWS, KV_HEADS, HEAD)
    seen = attention(q, k, v).reshape(ROWS, HEADS * HEAD)
    return (x.astype(jnp.float32) + jnp.dot(seen, wo, preferred_element_type=jnp.float32)).astype(jnp.bfloat16)
```

```python
import functools

import jax
import jax.numpy as jnp
from jax import lax
from jax.experimental import pallas as pl
from jax.experimental.pallas import tpu as pltpu
from jax.sharding import PartitionSpec as P

HEAD = 128
THETA = 10000
NEG = -1e30
HIDDEN = 2 * NEG
LOG2E = 1.4426950408889634
N = 16
T = 256
D = 4096
W = 256
HEADS = W // HEAD
SLOTS = 4
OSLOTS = 6
MESH = pl.DeviceIdType.MESH
BF = jnp.bfloat16
F32 = jnp.float32


def _xor(a, b):
    out = 0
    for bit in (1, 2, 4, 8):
        out = out + bit * lax.rem(lax.div(a, bit) + lax.div(b, bit), 2)
    return out


def _partner(me, i):
    half = 7 - lax.div(i, 2)
    return _xor(me, half + lax.rem(i, 2) * (15 - 2 * half))


def _dot(a, b, ca, cb):
    return lax.dot_general(a, b, (((ca,), (cb,)), ((), ())), preferred_element_type=F32)


def _kernel(x_ref, gain_ref, cos_ref, sin_ref, wk_ref, wv_ref, wq_ref, wo_ref, out_ref,
            a_s, w_s, stage_s, held_s, ostage_s, oheld_s, y_s, wo_s, top_s, mix_s,
            w_sem, wo_sem, send_sem, recv_sem, osend_sem, orecv_sem):
    me = lax.axis_index("sp")
    i32 = jnp.int32
    weights = (wk_ref, wv_ref, wq_ref)

    def fetch(t, i, slot):
        return pltpu.make_async_copy(weights[t].at[:, pl.ds(pl.multiple_of(_partner(me, i) * W, W), W)], w_s.at[slot], w_sem.at[slot])

    def fetch_out(i, slot):
        return pltpu.make_async_copy(wo_ref.at[pl.ds(pl.multiple_of(_partner(me, i) * W, W), W), :], wo_s.at[slot], wo_sem.at[slot])

    def send(t, there):
        return pltpu.make_async_remote_copy(stage_s.at[t, there], held_s.at[t, me], send_sem.at[t, there], recv_sem.at[t, me],
                                            device_id={"sp": there}, device_id_type=MESH)

    def arrive(t, there):
        return pltpu.make_async_remote_copy(stage_s.at[t, there], held_s.at[t, there], send_sem.at[t, there], recv_sem.at[t, there],
                                            device_id={"sp": there}, device_id_type=MESH)

    def send_out(there):
        return pltpu.make_async_remote_copy(ostage_s.at[there], oheld_s.at[me], osend_sem.at[there], orecv_sem.at[me],
                                            device_id={"sp": there}, device_id_type=MESH)

    def arrive_out(there):
        return pltpu.make_async_remote_copy(ostage_s.at[there], oheld_s.at[there], osend_sem.at[there], orecv_sem.at[there],
                                            device_id={"sp": there}, device_id_type=MESH)

    for n in range(SLOTS):
        fetch(0, jnp.int32(n), n).start()

    barrier = pltpu.get_barrier_semaphore()
    for o in range(1, N):
        pl.semaphore_signal(barrier, inc=1, device_id={"sp": lax.rem(me + o, N)}, device_id_type=MESH)

    def norm(r, z):
        rows = pl.ds(pl.multiple_of(r * 32, 32), 32)
        wide = x_ref[rows, :].astype(F32)
        scale = lax.rsqrt(jnp.mean(wide * wide, -1, keepdims=True) + 1e-6)
        a_s[rows, :] = (wide * scale * gain_ref[...].astype(F32)).astype(BF)
        y_s[rows, :] = wide
        return z

    lax.fori_loop(0, T // 32, norm, 0)
    pl.semaphore_wait(barrier, N - 1)

    def project(t):
        def body(i, z):
            n = t * N + i
            slot = lax.rem(n, SLOTS)
            there = _partner(me, i)
            fetch(t, i, slot).wait()
            p = jnp.dot(a_s[...], w_s[slot], preferred_element_type=F32).astype(BF)

            @pl.when(i + SLOTS < N)
            def _():
                fetch(t, i + SLOTS, slot).start()

            if t < 2:

                @pl.when(i + SLOTS >= N)
                def _():
                    fetch(t + 1, i + SLOTS - N, slot).start()

            if t == 1:
                p = p.T
            else:
                wide = p.astype(F32)
                parts = []
                for h in range(HEADS):
                    one = wide[:, h * HEAD : (h + 1) * HEAD]
                    parts.append(one * cos_ref[...] + pltpu.roll(one, HEAD // 2, 1) * sin_ref[...])
                p = jnp.concatenate(parts, axis=1).astype(BF)

            @pl.when(there == me)
            def _():
                held_s[t, me] = p

            @pl.when(there != me)
            def _():
                stage_s[t, there] = p
                send(t, there).start()

            return z

        lax.fori_loop(0, N, body, 0)

    project(0)
    project(1)
    project(2)
    for n in range(OSLOTS):
        fetch_out(jnp.int32(n), n).start()

    def await_kv(i, z):
        there = _partner(me, i)

        @pl.when(there != me)
        def _():
            arrive(0, there).wait_recv()
            arrive(1, there).wait_recv()

        return z

    lax.fori_loop(0, N, await_kv, 0)

    e = HEAD**-0.5 * LOG2E

    def attend(i, z):
        there = _partner(me, i)

        @pl.when(there != me)
        def _():
            arrive(2, there).wait_recv()

        top_s[...] = jnp.full(top_s.shape, NEG, F32)
        mix_s[...] = jnp.zeros(mix_s.shape, F32)
        ones = jnp.ones((8, T), BF)

        def block(j, masked):
            scores = []
            for h in range(HEADS):
                cols = slice(h * HEAD, (h + 1) * HEAD)
                q = held_s[2, there, :, cols]
                for u in range(2):
                    scores.append(_dot(held_s[0, 2 * j + u, :, cols], q, 1, 1))
            if masked:
                gap = lax.broadcasted_iota(i32, (T, T), 1) - lax.broadcasted_iota(i32, (T, T), 0)
                for u in range(2):
                    ok = gap >= (2 * j + u - there) * T
                    for h in range(HEADS):
                        scores[2 * h + u] = jnp.where(ok, scores[2 * h + u], HIDDEN)
            for h in range(HEADS):
                s0, s1 = scores[2 * h], scores[2 * h + 1]
                old = top_s[h : h + 1, :]
                top = jnp.maximum(old, jnp.maximum(s0, s1).max(axis=0, keepdims=True))
                top_s[h : h + 1, :] = top
                p0 = jnp.exp2((s0 - top) * e).astype(BF)
                p1 = jnp.exp2((s1 - top) * e).astype(BF)
                keep = jnp.exp2((old - top) * e)
                rows = slice(h * HEAD, (h + 1) * HEAD)
                v0 = jnp.concatenate([held_s[1, 2 * j, rows, :], ones], axis=0)
                v1 = jnp.concatenate([held_s[1, 2 * j + 1, rows, :], ones], axis=0)
                mix_s[h] = mix_s[h] * keep + _dot(v0, p0, 1, 0) + _dot(v1, p1, 1, 0)

        def whole(j, c):
            block(j, False)
            return c

        last = lax.div(there, 2)
        lax.fori_loop(0, last, whole, 0)
        block(last, True)
        parts = []
        for h in range(HEADS):
            total = mix_s[h, HEAD : HEAD + 1, :]
            parts.append((mix_s[h, :HEAD, :] * (1 / total)).T.astype(BF))
        o = jnp.concatenate(parts, axis=1)

        @pl.when(there == me)
        def _():
            oheld_s[me] = o

        @pl.when(there != me)
        def _():
            ostage_s[there] = o
            send_out(there).start()

        return z

    lax.fori_loop(0, N, attend, 0)

    C = 512

    def output(i, z):
        there = _partner(me, i)
        slot = lax.rem(i, OSLOTS)

        @pl.when(there != me)
        def _():
            arrive_out(there).wait_recv()

        fetch_out(i, slot).wait()

        def columns(c, z):
            cols = pl.ds(pl.multiple_of(c * C, C), C)
            y_s[:, cols] += jnp.dot(oheld_s[there], wo_s[slot, :, cols], preferred_element_type=F32)
            return z

        lax.fori_loop(0, D // C, columns, 0)

        @pl.when(i + OSLOTS < N)
        def _():
            fetch_out(i + OSLOTS, slot).start()

        return z

    lax.fori_loop(0, N, output, 0)
    out_ref[...] = y_s[...].astype(BF)

    def drain(i, z):
        there = _partner(me, i)

        @pl.when(there != me)
        def _():
            for t in range(3):
                send(t, there).wait_send()
            send_out(there).wait_send()

        return z

    lax.fori_loop(0, N, drain, 0)


def _tables(first):
    half = HEAD // 2
    lane = jnp.arange(HEAD)
    place = first + jnp.arange(T)
    angle = place.astype(F32)[:, None] * THETA ** (-(lane % half).astype(F32) / half)
    return jnp.cos(angle), jnp.where(lane < half, -jnp.sin(angle), jnp.sin(angle))


def solution(mesh):
    vmem, hbm = pl.BlockSpec(memory_space=pltpu.VMEM), pl.BlockSpec(memory_space=pl.ANY)

    def step(x, gain, wq, wk, wv, wo):
        cos, sin = _tables(lax.axis_index("sp") * T)
        dma = pltpu.SemaphoreType.DMA
        return pl.pallas_call(
            _kernel,
            out_shape=jax.ShapeDtypeStruct((T, D), BF),
            in_specs=[vmem, vmem, vmem, vmem, hbm, hbm, hbm, hbm],
            out_specs=vmem,
            scratch_shapes=[
                pltpu.VMEM((T, D), BF),
                pltpu.VMEM((SLOTS, D, W), BF),
                pltpu.VMEM((3, N, T, W), BF),
                pltpu.VMEM((3, N, T, W), BF),
                pltpu.VMEM((N, T, W), BF),
                pltpu.VMEM((N, T, W), BF),
                pltpu.VMEM((T, D), F32),
                pltpu.VMEM((OSLOTS, W, D), BF),
                pltpu.VMEM((8, T), F32),
                pltpu.VMEM((HEADS, HEAD + 8, T), F32),
                dma((SLOTS,)),
                dma((OSLOTS,)),
                dma((3, N)),
                dma((3, N)),
                dma((N,)),
                dma((N,)),
            ],
            compiler_params=pltpu.CompilerParams(collective_id=0, has_side_effects=True, vmem_limit_bytes=62 * 2**20),
        )(x, gain.reshape(1, D), cos, sin, wk, wv, wq, wo)

    tokens, whole = P(("dp", "sp"), None), P(None, None)
    return jax.shard_map(
        step,
        mesh=mesh,
        in_specs=(tokens, P(None), whole, whole, whole, whole),
        out_specs=tokens,
        check_vma=False,
    )
```

```python
import jax
import jax.numpy as jnp
import numpy as np
from jax import lax
from jax.experimental import pallas as pl
from jax.experimental.pallas import tpu as pltpu
from jax.sharding import PartitionSpec as P

HEAD = 128
THETA = 10000
NEG = -1e30
HIDDEN = 2 * NEG
LOG2E = 1.4426950408889634
N = 16
T = 256
D = 4096
W = 256
HEADS = W // HEAD
SLOTS = 4
OSLOTS = 4
PIECES = 8
C = D // PIECES
MESH = pl.DeviceIdType.MESH
BF = jnp.bfloat16
F32 = jnp.float32


def _xor(a, b):
    out = 0
    for bit in (1, 2, 4, 8):
        out = out + bit * lax.rem(lax.div(a, bit) + lax.div(b, bit), 2)
    return out


def _partner(me, i):
    half = 7 - lax.div(i, 2)
    return _xor(me, half + lax.rem(i, 2) * (15 - 2 * half))


def _dot(a, b, ca, cb):
    return lax.dot_general(a, b, (((ca,), (cb,)), ((), ())), preferred_element_type=F32)


def _kernel(x_ref, gain_ref, far_cos_ref, far_sin_ref, near_cos_ref, near_sin_ref, wk_ref, wv_ref, wq_ref, wo_ref, out_ref,
            x_s, a_s, cos_ref, sin_ref, w_s, stage_s, held_s, ostage_s, oheld_s, y_s, wo_s, even_s, odd_s, top_s, mix_s,
            x_sem, out_sem, w_sem, wo_sem, send_sem, recv_sem, osend_sem, orecv_sem):
    me = lax.axis_index("sp")
    i32 = jnp.int32
    weights = (wk_ref, wv_ref, wq_ref)

    def fetch(t, i, slot):
        return pltpu.make_async_copy(weights[t].at[:, pl.ds(pl.multiple_of(_partner(me, i) * W, W), W)], w_s.at[slot], w_sem.at[slot])

    def fetch_out(i, slot):
        return pltpu.make_async_copy(wo_ref.at[pl.ds(pl.multiple_of(_partner(me, i) * W, W), W), :], wo_s.at[slot], wo_sem.at[slot])

    def send(t, there):
        return pltpu.make_async_remote_copy(stage_s.at[t, there], held_s.at[t, me], send_sem.at[t, there], recv_sem.at[t, me],
                                            device_id={"sp": there}, device_id_type=MESH)

    def arrive(t, there):
        return pltpu.make_async_remote_copy(stage_s.at[t, there], held_s.at[t, there], send_sem.at[t, there], recv_sem.at[t, there],
                                            device_id={"sp": there}, device_id_type=MESH)

    def send_out(there):
        return pltpu.make_async_remote_copy(ostage_s.at[there], oheld_s.at[me], osend_sem.at[there], orecv_sem.at[me],
                                            device_id={"sp": there}, device_id_type=MESH)

    def arrive_out(there):
        return pltpu.make_async_remote_copy(ostage_s.at[there], oheld_s.at[there], osend_sem.at[there], orecv_sem.at[there],
                                            device_id={"sp": there}, device_id_type=MESH)

    get_x = pltpu.make_async_copy(x_ref, x_s, x_sem)
    get_x.start()
    for n in range(SLOTS):
        fetch(0, jnp.int32(n), n).start()

    barrier = pltpu.get_barrier_semaphore()
    for o in range(1, N):
        pl.semaphore_signal(barrier, inc=1, device_id={"sp": lax.rem(me + o, N)}, device_id_type=MESH)

    far_cos, far_sin = far_cos_ref[pl.ds(me, 1), :], far_sin_ref[pl.ds(me, 1), :]
    sign = jnp.where(lax.broadcasted_iota(i32, (T, HEAD), 1) < HEAD // 2, -1.0, 1.0).astype(F32)
    cos_ref[...] = far_cos * near_cos_ref[...] - far_sin * near_sin_ref[...]
    sin_ref[...] = (far_sin * near_cos_ref[...] + far_cos * near_sin_ref[...]) * sign
    gain = gain_ref[...].astype(F32).reshape(1, D)
    get_x.wait()

    def norm(r, z):
        rows = pl.ds(pl.multiple_of(r * 32, 32), 32)
        wide = x_s[rows, :].astype(F32)
        scale = lax.rsqrt(jnp.mean(wide * wide, -1, keepdims=True) + 1e-6)
        a_s[rows, :] = (wide * scale * gain).astype(BF)
        return z

    lax.fori_loop(0, T // 32, norm, 0)

    def project(t):
        def body(i, z):
            n = t * N + i
            slot = lax.rem(n, SLOTS)
            there = _partner(me, i)
            fetch(t, i, slot).wait()
            p = jnp.dot(a_s[...], w_s[slot], preferred_element_type=F32).astype(BF)

            @pl.when(i + SLOTS < N)
            def _():
                fetch(t, i + SLOTS, slot).start()

            if t < 2:

                @pl.when(i + SLOTS >= N)
                def _():
                    fetch(t + 1, i + SLOTS - N, slot).start()

            if t == 1:
                p = p.T
            else:
                wide = p.astype(F32)
                parts = []
                for h in range(HEADS):
                    one = wide[:, h * HEAD : (h + 1) * HEAD]
                    parts.append(one * cos_ref[...] + pltpu.roll(one, HEAD // 2, 1) * sin_ref[...])
                p = jnp.concatenate(parts, axis=1).astype(BF)
                if t == 2:
                    p = p.T

            if t == 0:

                @pl.when(i == 0)
                def _():
                    pl.semaphore_wait(barrier, N - 1)

            @pl.when(there == me)
            def _():
                held_s[t, me] = p

            @pl.when(there != me)
            def _():
                stage_s[t, there] = p
                send(t, there).start()

            return z

        lax.fori_loop(0, N, body, 0)

    project(0)
    project(1)
    project(2)
    for n in range(OSLOTS):
        fetch_out(jnp.int32(n), n).start()

    y_s[...] = x_s[...].astype(F32)

    def await_kv(i, z):
        there = _partner(me, i)

        @pl.when(there != me)
        def _():
            arrive(0, there).wait_recv()
            arrive(1, there).wait_recv()

        return z

    lax.fori_loop(0, N, await_kv, 0)

    e = HEAD**-0.5 * LOG2E

    def attend(i, z):
        there = _partner(me, i)

        @pl.when(there != me)
        def _():
            arrive(2, there).wait_recv()

        top_s[...] = jnp.full(top_s.shape, NEG, F32)
        mix_s[...] = jnp.zeros(mix_s.shape, F32)
        ones = jnp.ones((8, T), BF)

        def score(j, buf):
            for h in range(HEADS):
                part = slice(h * HEAD, (h + 1) * HEAD)
                k = held_s[0, pl.ds(2 * j, 2), :, part].reshape(2 * T, HEAD)
                buf[h] = _dot(k, held_s[2, there, part, :], 1, 0)

        def take(j, buf, masked):
            for h in range(HEADS):
                s = buf[h]
                if masked:
                    gap = lax.broadcasted_iota(i32, s.shape, 1) - lax.broadcasted_iota(i32, s.shape, 0)
                    s = jnp.where(gap >= (2 * j - there) * T, s, HIDDEN)
                old = top_s[h : h + 1, :]
                top = jnp.maximum(old, s.max(axis=0, keepdims=True))
                top_s[h : h + 1, :] = top
                p = jnp.exp2((s - top) * e).astype(BF)
                keep = jnp.exp2((old - top) * e)
                mix = mix_s[h] * keep
                for u in range(2):
                    v = jnp.concatenate([held_s[1, 2 * j + u, h * HEAD : (h + 1) * HEAD, :], ones], axis=0)
                    mix += _dot(v, p[u * T : (u + 1) * T, :], 1, 0)
                mix_s[h] = mix

        def two(jj, z):
            j = 2 * jj
            score(j + 1, odd_s)
            take(j, even_s, False)
            score(j + 2, even_s)
            take(j + 1, odd_s, False)
            return z

        last = lax.div(there, 2)
        score(0, even_s)
        lax.fori_loop(0, lax.div(last, 2), two, 0)

        @pl.when(lax.rem(last, 2) == 0)
        def _():
            take(last, even_s, True)

        @pl.when(lax.rem(last, 2) == 1)
        def _():
            score(last, odd_s)
            take(last - 1, even_s, False)
            take(last, odd_s, True)

        parts = []
        for h in range(HEADS):
            total = mix_s[h, HEAD : HEAD + 1, :]
            parts.append((mix_s[h, :HEAD, :] * (1 / total)).T.astype(BF))
        o = jnp.concatenate(parts, axis=1)

        @pl.when(there == me)
        def _():
            oheld_s[me] = o

        @pl.when(there != me)
        def _():
            ostage_s[there] = o
            send_out(there).start()

        return z

    lax.fori_loop(0, N, attend, 0)

    def output(i, last):
        there = _partner(me, i)
        slot = lax.rem(i, OSLOTS)

        @pl.when(there != me)
        def _():
            arrive_out(there).wait_recv()

        fetch_out(i, slot).wait()
        o = oheld_s[there]
        for c in range(PIECES):
            cols = slice(c * C, (c + 1) * C)
            y = y_s[:, cols] + jnp.dot(o, wo_s[slot, :, cols], preferred_element_type=F32)
            if last:
                x_s[:, cols] = y.astype(BF)
                pltpu.make_async_copy(x_s.at[:, cols], out_ref.at[:, cols], out_sem.at[c]).start()
            else:
                y_s[:, cols] = y

        if not last:

            @pl.when(i + OSLOTS < N)
            def _():
                fetch_out(i + OSLOTS, slot).start()

    def output_step(i, z):
        output(i, False)
        return z

    lax.fori_loop(0, N - 1, output_step, 0)
    output(jnp.int32(N - 1), True)

    def drain(i, z):
        there = _partner(me, i)

        @pl.when(there != me)
        def _():
            for t in range(3):
                send(t, there).wait_send()
            send_out(there).wait_send()

        return z

    lax.fori_loop(0, N, drain, 0)
    for c in range(PIECES):
        cols = slice(c * C, (c + 1) * C)
        pltpu.make_async_copy(x_s.at[:, cols], out_ref.at[:, cols], out_sem.at[c]).wait()


def _tables():
    half = HEAD // 2
    lane = np.arange(HEAD)
    rate = THETA ** (-(lane % half).astype(np.float64) / half)
    far, near = (np.arange(N) * T)[:, None] * rate, np.arange(T)[:, None] * rate
    return [jnp.asarray(f(x), F32) for x in (far, near) for f in (np.cos, np.sin)]


def solution(mesh):
    vmem, hbm = pl.BlockSpec(memory_space=pltpu.VMEM), pl.BlockSpec(memory_space=pl.ANY)

    def step(x, gain, wq, wk, wv, wo):
        dma = pltpu.SemaphoreType.DMA
        return pl.pallas_call(
            _kernel,
            out_shape=jax.ShapeDtypeStruct((T, D), BF),
            in_specs=[hbm] + [vmem] * 5 + [hbm] * 4,
            out_specs=hbm,
            scratch_shapes=[
                pltpu.VMEM((T, D), BF),
                pltpu.VMEM((T, D), BF),
                pltpu.VMEM((T, HEAD), F32),
                pltpu.VMEM((T, HEAD), F32),
                pltpu.VMEM((SLOTS, D, W), BF),
                pltpu.VMEM((3, N, T, W), BF),
                pltpu.VMEM((3, N, T, W), BF),
                pltpu.VMEM((N, T, W), BF),
                pltpu.VMEM((N, T, W), BF),
                pltpu.VMEM((T, D), F32),
                pltpu.VMEM((OSLOTS, W, D), BF),
                pltpu.VMEM((HEADS, 2 * T, T), F32),
                pltpu.VMEM((HEADS, 2 * T, T), F32),
                pltpu.VMEM((8, T), F32),
                pltpu.VMEM((HEADS, HEAD + 8, T), F32),
                dma,
                dma((PIECES,)),
                dma((SLOTS,)),
                dma((OSLOTS,)),
                dma((3, N)),
                dma((3, N)),
                dma((N,)),
                dma((N,)),
            ],
            compiler_params=pltpu.CompilerParams(collective_id=0, has_side_effects=True, vmem_limit_bytes=62 * 2**20),
        )(x, gain, *_tables(), wk, wv, wq, wo)

    tokens, whole = P(("dp", "sp"), None), P(None, None)
    return jax.shard_map(
        step,
        mesh=mesh,
        in_specs=(tokens, P(None), whole, whole, whole, whole),
        out_specs=tokens,
        check_vma=False,
    )
```

```python
import jax
import jax.numpy as jnp
import numpy as np
from jax import lax
from jax.experimental import pallas as pl
from jax.experimental.pallas import tpu as pltpu
from jax.sharding import PartitionSpec as P

HEAD = 128
THETA = 10000
NEG = -1e30
HIDDEN = 2 * NEG
LOG2E = 1.4426950408889634
N = 16
CHIPS = N // 2
STEPS = CHIPS // 2
T = 256
D = 4096
W = 256
HEADS = W // HEAD
SLOTS = 3
OSLOTS = 4
PIECES = 8
C = D // PIECES
MESH = pl.DeviceIdType.MESH
BF = jnp.bfloat16
F32 = jnp.float32
E = HEAD**-0.5 * LOG2E


def _xor(a, b):
    out = 0
    for bit in (1, 2, 4):
        out = out + bit * lax.rem(lax.div(a, bit) + lax.div(b, bit), 2)
    return out


def _met(chip, i):
    low = 3 - lax.div(i, 2)
    return _xor(chip, low + lax.rem(i, 2) * (7 - 2 * low))


def _dot(a, b):
    return jnp.dot(a, b, preferred_element_type=F32)


def _kernel(x_ref, gain_ref, table_ref, wk_ref, wv_ref, wq_ref, wo_ref, out_ref,
            x_s, gain_s, table_s, a_s, cos_s, sin_s, w_s, kstage_s, stage_s, k_s, vq_s, ostage_s, o_s, y_s, wo_s, even_s, odd_s, top_s, mix_s,
            x_sem, w_sem, wo_sem, send_sem, recv_sem, osend_sem, orecv_sem):
    me = lax.axis_index("sp")
    chip = lax.div(me, 2)
    i32 = jnp.int32
    weights = (wk_ref, wv_ref, wq_ref)

    def fetch(stage, i, slot):
        for n in range(4):
            at = pl.multiple_of((2 * _met(chip, 2 * i + n // 2) + n % 2) * W + stage // 3 * HEAD, HEAD)
            yield pltpu.make_async_copy(weights[stage % 3].at[:, pl.ds(at, HEAD)], w_s.at[slot, :, n * HEAD : (n + 1) * HEAD], w_sem.at[slot, n])

    def start(copies):
        for one in copies:
            one.start()

    def fetch_out(h, i, u, slot):
        at = pl.multiple_of((2 * _met(chip, i) + u) * W + h * HEAD, HEAD)
        return pltpu.make_async_copy(wo_ref.at[pl.ds(at, HEAD), :], wo_s.at[slot, pl.ds(u * HEAD, HEAD)], wo_sem.at[slot, u])

    def copy(t, h, there, place):
        src = kstage_s.at[there, h] if t == 0 else stage_s.at[t - 1, there, h]
        dst = k_s.at[h, place] if t == 0 else vq_s.at[t - 1, h, place]
        return pltpu.make_async_remote_copy(src, dst, send_sem.at[t, h, there], recv_sem.at[t, h, place], device_id={"sp": there}, device_id_type=MESH)

    def copy_out(h, there, place):
        return pltpu.make_async_remote_copy(ostage_s.at[h, there], o_s.at[h, place], osend_sem.at[h, there], orecv_sem.at[h, place],
                                            device_id={"sp": there}, device_id_type=MESH)

    first = [pltpu.make_async_copy(a, b, x_sem.at[n]) for n, (a, b) in enumerate(((x_ref, x_s), (table_ref, table_s), (gain_ref, gain_s)))]
    for one in first:
        one.start()

    barrier = pltpu.get_barrier_semaphore()
    for o in range(1, N):
        pl.semaphore_signal(barrier, inc=1, device_id={"sp": lax.rem(me + o, N)}, device_id_type=MESH)

    for one in first:
        one.wait()
    for n in range(SLOTS):
        start(fetch(0, jnp.int32(n), n))
    gain = gain_s[...].astype(F32).reshape(1, D)

    def norm(r, z):
        rows = pl.ds(pl.multiple_of(r * 32, 32), 32)
        wide = x_s[rows, :].astype(F32)
        scale = lax.rsqrt(jnp.mean(wide * wide, -1, keepdims=True) + 1e-6)
        a_s[rows, :] = (wide * scale * gain).astype(BF)
        return z

    lax.fori_loop(0, T // 32, norm, 0)
    far_cos, far_sin = table_s[0, pl.ds(me, 1), :], table_s[1, pl.ds(me, 1), :]
    near_cos, near_sin = table_s[0, N:, :], table_s[1, N:, :]
    sign = jnp.where(lax.broadcasted_iota(i32, (T, HEAD), 1) < HEAD // 2, -1.0, 1.0).astype(F32)
    cos_s[...] = far_cos * near_cos - far_sin * near_sin
    sin_s[...] = (far_sin * near_cos + far_cos * near_sin) * sign

    def project(stage):
        h, t = stage // 3, stage % 3

        def body(i, z):
            slot = lax.rem(stage * STEPS + i, SLOTS)
            for one in fetch(stage, i, slot):
                one.wait()
            for v in range(2):
                pair = _met(chip, 2 * i + v)
                p = _dot(a_s[...], w_s[slot, :, v * W : (v + 1) * W]).astype(BF)
                for u in range(2):
                    one = p[:, u * HEAD : (u + 1) * HEAD]
                    if t != 1:
                        wide = one.astype(F32)
                        one = (wide * cos_s[...] + pltpu.roll(wide, HEAD // 2, 1) * sin_s[...]).astype(BF)
                    if t == 0:
                        kstage_s[2 * pair + u, h] = one
                    else:
                        stage_s[t - 1, 2 * pair + u, h] = one.T

            @pl.when(i + SLOTS < STEPS)
            def _():
                start(fetch(stage, i + SLOTS, slot))

            if stage < 5:

                @pl.when(i + SLOTS >= STEPS)
                def _():
                    start(fetch(stage + 1, i + SLOTS - STEPS, slot))

            if stage == 0:

                @pl.when(i == 0)
                def _():
                    pl.semaphore_wait(barrier, N - 1)

            for n in range(4):
                there = 2 * _met(chip, 2 * i + n // 2) + n % 2

                @pl.when(there != me)
                def _():
                    copy(t, h, there, me).start()

                @pl.when(there == me)
                def _():
                    if t == 0:
                        k_s[h, me] = kstage_s[me, h]
                    else:
                        vq_s[t - 1, h, me] = stage_s[t - 1, me, h]

            return z

        lax.fori_loop(0, STEPS, body, 0)

    def others(i, do):
        for u in range(2):
            there = 2 * _met(chip, i) + u

            @pl.when(there != me)
            def _():
                do(there)

    def each(do):
        def body(i, z):
            others(i, do)
            return z

        lax.fori_loop(0, CHIPS, body, 0)

    project(0)
    project(1)
    project(2)
    project(3)
    project(4)
    project(5)
    for n in range(OSLOTS):
        for u in range(2):
            fetch_out(0, jnp.int32(n), u, n).start()
    y_s[...] = x_s[...].astype(F32)

    def output(h, i, last):
        pair = _met(chip, i)
        slot = lax.rem(i, OSLOTS)
        for u in range(2):
            there = 2 * pair + u

            @pl.when(there != me)
            def _():
                copy_out(h, there, there).wait_recv()

            fetch_out(h, i, u, slot).wait()
        o = jnp.concatenate([o_s[h, 2 * pair], o_s[h, 2 * pair + 1]], axis=1)
        for c in range(PIECES):
            cols = slice(c * C, (c + 1) * C)
            y = y_s[:, cols] + _dot(o, wo_s[slot, :, cols])
            if last:
                out_ref[:, cols] = y.astype(BF)
            else:
                y_s[:, cols] = y

        if not last:

            @pl.when(i + OSLOTS < CHIPS)
            def _():
                for u in range(2):
                    fetch_out(h, i + OSLOTS, u, slot).start()

            if h == 0:

                @pl.when(i + OSLOTS >= CHIPS)
                def _():
                    for u in range(2):
                        fetch_out(1, i + OSLOTS - CHIPS, u, slot).start()

    def attend(h):
        def await_kv(there):
            copy(0, h, there, there).wait_recv()
            copy(1, h, there, there).wait_recv()

        each(await_kv)
        if h == 1:
            each(lambda there: copy_out(0, there, me).start())

        def body(i, z):
            pair = _met(chip, i)
            others(i, lambda there: copy(2, h, there, there).wait_recv())
            top_s[...] = jnp.full(top_s.shape, NEG, F32)
            mix_s[...] = jnp.zeros(mix_s.shape, F32)
            ones = jnp.ones((8, T), BF)

            def score(j, buf):
                k = k_s[h, pl.ds(2 * j, 2)].reshape(2 * T, HEAD)
                for u in range(2):
                    buf[u] = _dot(k, vq_s[1, h, 2 * pair + u])

            def take(j, buf, masked):
                for u in range(2):
                    parts = u + 1 if masked else 2
                    s = buf[u, : parts * T]
                    if masked:
                        gap = lax.broadcasted_iota(i32, s.shape, 1) - lax.broadcasted_iota(i32, s.shape, 0)
                        s = jnp.where(gap >= -u * T, s, HIDDEN)
                    old = top_s[u : u + 1, :]
                    top = jnp.maximum(old, s.max(axis=0, keepdims=True))
                    top_s[u : u + 1, :] = top
                    p = jnp.exp2((s - top) * E).astype(BF)
                    keep = jnp.exp2((old - top) * E)
                    mix = mix_s[u] * keep
                    for n in range(parts):
                        v = jnp.concatenate([vq_s[0, h, 2 * j + n], ones], axis=0)
                        mix += _dot(v, p[n * T : (n + 1) * T, :])
                    mix_s[u] = mix

            def two(jj, z):
                j = 2 * jj
                score(j + 1, odd_s)
                take(j, even_s, False)
                score(j + 2, even_s)
                take(j + 1, odd_s, False)
                return z

            score(0, even_s)
            lax.fori_loop(0, lax.div(pair, 2), two, 0)

            @pl.when(lax.rem(pair, 2) == 0)
            def _():
                take(pair, even_s, True)

            @pl.when(lax.rem(pair, 2) == 1)
            def _():
                score(pair, odd_s)
                take(pair - 1, even_s, False)
                take(pair, odd_s, True)

            for u in range(2):
                there = 2 * pair + u
                o = (mix_s[u, :HEAD, :] * (1 / mix_s[u, HEAD : HEAD + 1, :])).astype(BF).T
                ostage_s[h, there] = o

            for u in range(2):
                there = 2 * pair + u

                @pl.when(there == me)
                def _():
                    o_s[h, me] = ostage_s[h, me]

                if h == 1:

                    @pl.when(there != me)
                    def _():
                        copy_out(1, there, me).start()

            return z

        lax.fori_loop(0, CHIPS, body, 0)

    attend(0)
    attend(1)

    for h in range(HEADS):

        def output_step(i, z):
            output(h, i, False)
            return z

        lax.fori_loop(0, CHIPS - h, output_step, 0)

    def drain(there):
        for h in range(HEADS):
            for t in range(3):
                copy(t, h, there, me).wait_send()
        copy_out(0, there, me).wait_send()

    each(drain)
    output(1, jnp.int32(CHIPS - 1), True)
    each(lambda there: copy_out(1, there, me).wait_send())


def _table():
    half = HEAD // 2
    rate = THETA ** (-(np.arange(HEAD) % half).astype(np.float64) / half)
    angle = np.concatenate([np.arange(N) * T, np.arange(T)])[:, None] * rate
    return jnp.asarray(np.stack([np.cos(angle), np.sin(angle)]), F32)


def solution(mesh):
    def step(x, gain, wq, wk, wv, wo):
        dma = pltpu.SemaphoreType.DMA
        return pl.pallas_call(
            _kernel,
            out_shape=pltpu.VMEM((T, D), BF),
            in_specs=[pl.BlockSpec(memory_space=pltpu.HBM)] * 7,
            out_specs=pl.BlockSpec(memory_space=pltpu.VMEM),
            scratch_shapes=[
                pltpu.VMEM((T, D), BF),
                pltpu.VMEM((D,), BF),
                pltpu.VMEM((2, N + T, HEAD), F32),
                pltpu.VMEM((T, D), BF),
                pltpu.VMEM((T, HEAD), F32),
                pltpu.VMEM((T, HEAD), F32),
                pltpu.VMEM((SLOTS, D, 2 * W), BF),
                pltpu.VMEM((N, HEADS, T, HEAD), BF),
                pltpu.VMEM((2, N, HEADS, HEAD, T), BF),
                pltpu.VMEM((HEADS, N, T, HEAD), BF),
                pltpu.VMEM((2, HEADS, N, HEAD, T), BF),
                pltpu.VMEM((HEADS, N, T, HEAD), BF),
                pltpu.VMEM((HEADS, N, T, HEAD), BF),
                pltpu.VMEM((T, D), F32),
                pltpu.VMEM((OSLOTS, 2 * HEAD, D), BF),
                pltpu.VMEM((2, 2 * T, T), F32),
                pltpu.VMEM((2, 2 * T, T), F32),
                pltpu.VMEM((8, T), F32),
                pltpu.VMEM((2, HEAD + 8, T), F32),
                dma((3,)),
                dma((SLOTS, 4)),
                dma((OSLOTS, 2)),
                dma((3, HEADS, N)),
                dma((3, HEADS, N)),
                dma((HEADS, N)),
                dma((HEADS, N)),
            ],
            compiler_params=pltpu.CompilerParams(collective_id=0, has_side_effects=True, vmem_limit_bytes=49 * 2**20),
        )(*(pltpu.with_memory_space_constraint(t, pltpu.HBM) for t in (x, gain, _table(), wk, wv, wq, wo)))

    tokens, whole = P(("dp", "sp"), None), P(None, None)
    return jax.shard_map(
        step,
        mesh=mesh,
        in_specs=(tokens, P(None), whole, whole, whole, whole),
        out_specs=tokens,
        check_vma=False,
    )
```

```python
import jax
import jax.numpy as jnp
import numpy as np
from jax import lax
from jax.experimental import pallas as pl
from jax.experimental.pallas import tpu as pltpu
from jax.sharding import PartitionSpec as P

HEAD = 128
THETA = 10000
NEG = -1e30
HIDDEN = 2 * NEG
LOG2E = 1.4426950408889634
N = 16
ORDER = ((0, 0), (0, 1), (0, 2), (1, 2), (1, 0), (1, 1))
CHIPS = N // 2
STEPS = CHIPS // 2
T = 256
D = 4096
W = 256
HEADS = W // HEAD
SLOTS = 3
OSLOTS = 4
PIECES = 8
C = D // PIECES
MESH = pl.DeviceIdType.MESH
BF = jnp.bfloat16
F32 = jnp.float32
E = HEAD**-0.5 * LOG2E


def _xor(a, b):
    out = 0
    for bit in (1, 2, 4):
        out = out + bit * lax.rem(lax.div(a, bit) + lax.div(b, bit), 2)
    return out


def _met(chip, i):
    step = lax.div(i, 2)
    even = 1 + step + lax.div(step, 2) - 5 * lax.div(step, 3)
    return _xor(chip, even + lax.rem(i, 2) * (7 - 2 * even))


def _dot(a, b):
    return jnp.dot(a, b, preferred_element_type=F32)


def _kernel(x_ref, gain_ref, table_ref, wk_ref, wv_ref, wq_ref, wo_ref, out_ref,
            x_s, gain_s, table_s, a_s, cos_s, sin_s, w_s, kstage_s, stage_s, k_s, vq_s, ostage_s, o_s, y_s, wo_s, even_s, odd_s, top_s, mix_s,
            x_sem, w_sem, wo_sem, send_sem, recv_sem, osend_sem, orecv_sem):
    me = lax.axis_index("sp")
    chip = lax.div(me, 2)
    i32 = jnp.int32
    weights = (wk_ref, wv_ref, wq_ref)

    def fetch(stage, i, slot):
        h, t = ORDER[stage]
        for n in range(4):
            at = pl.multiple_of((2 * _met(chip, 2 * i + n // 2) + n % 2) * W + h * HEAD, HEAD)
            yield pltpu.make_async_copy(weights[t].at[:, pl.ds(at, HEAD)], w_s.at[slot, :, n * HEAD : (n + 1) * HEAD], w_sem.at[slot, n])

    def start(copies):
        for one in copies:
            one.start()

    def fetch_out(h, i, u, slot):
        at = pl.multiple_of((2 * _met(chip, i) + u) * W + h * HEAD, HEAD)
        return pltpu.make_async_copy(wo_ref.at[pl.ds(at, HEAD), :], wo_s.at[slot, pl.ds(u * HEAD, HEAD)], wo_sem.at[slot, u])

    def copy(t, h, there, place):
        src = kstage_s.at[there, h] if t == 0 else stage_s.at[t - 1, there, h]
        dst = k_s.at[h, place] if t == 0 else vq_s.at[t - 1, h, place]
        return pltpu.make_async_remote_copy(src, dst, send_sem.at[t, h, there], recv_sem.at[t, h, place], device_id={"sp": there}, device_id_type=MESH)

    def copy_out(h, there, place):
        return pltpu.make_async_remote_copy(ostage_s.at[h, there], o_s.at[h, place], osend_sem.at[h, there], orecv_sem.at[h, place],
                                            device_id={"sp": there}, device_id_type=MESH)

    first = [pltpu.make_async_copy(a, b, x_sem.at[n]) for n, (a, b) in enumerate(((x_ref, x_s), (table_ref, table_s), (gain_ref, gain_s)))]
    for one in first:
        one.start()

    barrier = pltpu.get_barrier_semaphore()
    for o in range(1, N):
        pl.semaphore_signal(barrier, inc=1, device_id={"sp": lax.rem(me + o, N)}, device_id_type=MESH)

    for one in first:
        one.wait()
    for n in range(SLOTS):
        start(fetch(0, jnp.int32(n), n))
    gain = gain_s[...].astype(F32).reshape(1, D)

    def norm(r, z):
        rows = pl.ds(pl.multiple_of(r * 32, 32), 32)
        wide = x_s[rows, :].astype(F32)
        scale = lax.rsqrt(jnp.mean(wide * wide, -1, keepdims=True) + 1e-6)
        a_s[rows, :] = (wide * scale * gain).astype(BF)
        return z

    lax.fori_loop(0, T // 32, norm, 0)
    far_cos, far_sin = table_s[0, pl.ds(me, 1), :], table_s[1, pl.ds(me, 1), :]
    near_cos, near_sin = table_s[0, N:, :], table_s[1, N:, :]
    sign = jnp.where(lax.broadcasted_iota(i32, (T, HEAD), 1) < HEAD // 2, -1.0, 1.0).astype(F32)
    cos_s[...] = far_cos * near_cos - far_sin * near_sin
    sin_s[...] = (far_sin * near_cos + far_cos * near_sin) * sign

    def project(stage):
        h, t = ORDER[stage]

        def body(i, z):
            slot = lax.rem(stage * STEPS + i, SLOTS)
            for one in fetch(stage, i, slot):
                one.wait()
            for v in range(2):
                pair = _met(chip, 2 * i + v)
                p = _dot(a_s[...], w_s[slot, :, v * W : (v + 1) * W]).astype(BF)
                for u in range(2):
                    one = p[:, u * HEAD : (u + 1) * HEAD]
                    if t != 1:
                        wide = one.astype(F32)
                        one = (wide * cos_s[...] + pltpu.roll(wide, HEAD // 2, 1) * sin_s[...]).astype(BF)
                    if t == 0:
                        kstage_s[2 * pair + u, h] = one
                    else:
                        stage_s[t - 1, 2 * pair + u, h] = one.T

            @pl.when(i + SLOTS < STEPS)
            def _():
                start(fetch(stage, i + SLOTS, slot))

            if stage < 5:

                @pl.when(i + SLOTS >= STEPS)
                def _():
                    start(fetch(stage + 1, i + SLOTS - STEPS, slot))

            if stage == 0:

                @pl.when(i == 0)
                def _():
                    pl.semaphore_wait(barrier, N - 1)

            for n in range(4):
                there = 2 * _met(chip, 2 * i + n // 2) + n % 2

                if (h, t) != (1, 0):

                    @pl.when(there != me)
                    def _():
                        if (h, t) == (1, 1):
                            copy(0, 1, there, me).start()
                        copy(t, h, there, me).start()

                @pl.when(there == me)
                def _():
                    if t == 0:
                        k_s[h, me] = kstage_s[me, h]
                    else:
                        vq_s[t - 1, h, me] = stage_s[t - 1, me, h]

            return z

        lax.fori_loop(0, STEPS, body, 0)

    def others(i, do):
        for u in range(2):
            there = 2 * _met(chip, i) + u

            @pl.when(there != me)
            def _():
                do(there)

    def each(do):
        def body(i, z):
            others(i, do)
            return z

        lax.fori_loop(0, CHIPS, body, 0)

    project(0)
    project(1)
    project(2)
    project(3)
    project(4)
    project(5)
    for n in range(OSLOTS):
        for u in range(2):
            fetch_out(0, jnp.int32(n), u, n).start()
    y_s[...] = x_s[...].astype(F32)

    def output(h, i, last):
        pair = _met(chip, i)
        slot = lax.rem(i, OSLOTS)
        for u in range(2):
            there = 2 * pair + u

            @pl.when(there != me)
            def _():
                copy_out(h, there, there).wait_recv()

            fetch_out(h, i, u, slot).wait()
        o = jnp.concatenate([o_s[h, 2 * pair], o_s[h, 2 * pair + 1]], axis=1)
        for c in range(PIECES):
            cols = slice(c * C, (c + 1) * C)
            y = y_s[:, cols] + _dot(o, wo_s[slot, :, cols])
            if last:
                out_ref[:, cols] = y.astype(BF)
            else:
                y_s[:, cols] = y

        if not last:

            @pl.when(i + OSLOTS < CHIPS)
            def _():
                for u in range(2):
                    fetch_out(h, i + OSLOTS, u, slot).start()

            if h == 0:

                @pl.when(i + OSLOTS >= CHIPS)
                def _():
                    for u in range(2):
                        fetch_out(1, i + OSLOTS - CHIPS, u, slot).start()

    ones = jnp.ones((8, T), BF)

    def score(h, pair, j, buf):
        k = k_s[h, pl.ds(2 * j, 2)].reshape(2 * T, HEAD)
        for u in range(2):
            buf[u] = _dot(k, vq_s[1, h, 2 * pair + u])

    def take(h, pair, j, buf, masked):
        for u in range(2):
            parts = u + 1 if masked else 2
            s = buf[u, : parts * T]
            if masked:
                gap = lax.broadcasted_iota(i32, s.shape, 1) - lax.broadcasted_iota(i32, s.shape, 0)
                s = jnp.where(gap >= -u * T, s, HIDDEN)
            old = top_s[pair, u : u + 1, :]
            top = jnp.maximum(old, s.max(axis=0, keepdims=True))
            top_s[pair, u : u + 1, :] = top
            p = jnp.exp2((s - top) * E).astype(BF)
            keep = jnp.exp2((old - top) * E)
            mix = mix_s[pair, u] * keep
            for n in range(parts):
                v = jnp.concatenate([vq_s[0, h, 2 * j + n], ones], axis=0)
                mix += _dot(v, p[n * T : (n + 1) * T, :])
            mix_s[pair, u] = mix

    def clear():
        top_s[...] = jnp.full(top_s.shape, NEG, F32)

        def body(pair, z):
            mix_s[pair] = jnp.zeros(mix_s.shape[1:], F32)
            return z

        lax.fori_loop(0, CHIPS, body, 0)

    def finish(h, pair):
        for u in range(2):
            o = (mix_s[pair, u, :HEAD, :] * (1 / mix_s[pair, u, HEAD : HEAD + 1, :])).astype(BF).T
            ostage_s[h, 2 * pair + u] = o

        for u in range(2):
            there = 2 * pair + u

            @pl.when(there == me)
            def _():
                o_s[h, me] = ostage_s[h, me]

            @pl.when(there != me)
            def _():
                copy_out(h, there, me).start()

    def await_all(h, t):
        each(lambda there: copy(t, h, there, there).wait_recv())

    def by_queries(i, z):
        pair = _met(chip, i)
        others(i, lambda there: copy(2, 0, there, there).wait_recv())

        def two(n, z):
            j = 2 * n
            score(0, pair, j + 1, odd_s)
            take(0, pair, j, even_s, False)
            score(0, pair, j + 2, even_s)
            take(0, pair, j + 1, odd_s, False)
            return z

        score(0, pair, 0, even_s)
        lax.fori_loop(0, lax.div(pair, 2), two, 0)

        @pl.when(lax.rem(pair, 2) == 0)
        def _():
            take(0, pair, pair, even_s, True)

        @pl.when(lax.rem(pair, 2) == 1)
        def _():
            score(0, pair, pair, odd_s)
            take(0, pair, pair - 1, even_s, False)
            take(0, pair, pair, odd_s, True)

        finish(0, pair)
        return z

    def by_keys(i, z):
        j = _met(chip, i)

        def await_pair(there):
            copy(0, 1, there, there).wait_recv()
            copy(1, 1, there, there).wait_recv()

        others(i, await_pair)
        score(1, j, j, even_s)
        score(1, jnp.minimum(j + 1, CHIPS - 1), j, odd_s)
        take(1, j, j, even_s, True)

        def two(n, z):
            pair = j + 1 + 2 * n
            score(1, pair + 1, j, even_s)
            take(1, pair, j, odd_s, False)
            score(1, jnp.minimum(pair + 2, CHIPS - 1), j, odd_s)
            take(1, pair + 1, j, even_s, False)
            return z

        rest = CHIPS - 1 - j
        lax.fori_loop(0, lax.div(rest, 2), two, 0)

        @pl.when(lax.rem(rest, 2) == 1)
        def _():
            take(1, CHIPS - 1, j, odd_s, False)

        return z

    def finish_step(i, z):
        finish(1, _met(chip, i))
        return z

    clear()
    await_all(0, 0)
    await_all(0, 1)
    lax.fori_loop(0, CHIPS, by_queries, 0)
    clear()
    await_all(1, 2)
    lax.fori_loop(0, CHIPS, by_keys, 0)
    lax.fori_loop(0, CHIPS, finish_step, 0)

    for h in range(HEADS):

        def output_step(i, z):
            output(h, i, False)
            return z

        lax.fori_loop(0, CHIPS - h, output_step, 0)

    def drain(there):
        for h in range(HEADS):
            for t in range(3):
                copy(t, h, there, me).wait_send()
        copy_out(0, there, me).wait_send()

    each(drain)
    output(1, jnp.int32(CHIPS - 1), True)
    each(lambda there: copy_out(1, there, me).wait_send())


def _table():
    half = HEAD // 2
    rate = THETA ** (-(np.arange(HEAD) % half).astype(np.float64) / half)
    angle = np.concatenate([np.arange(N) * T, np.arange(T)])[:, None] * rate
    return jnp.asarray(np.stack([np.cos(angle), np.sin(angle)]), F32)


def solution(mesh):
    def step(x, gain, wq, wk, wv, wo):
        dma = pltpu.SemaphoreType.DMA
        return pl.pallas_call(
            _kernel,
            out_shape=pltpu.VMEM((T, D), BF),
            in_specs=[pl.BlockSpec(memory_space=pltpu.HBM)] * 7,
            out_specs=pl.BlockSpec(memory_space=pltpu.VMEM),
            scratch_shapes=[
                pltpu.VMEM((T, D), BF),
                pltpu.VMEM((D,), BF),
                pltpu.VMEM((2, N + T, HEAD), F32),
                pltpu.VMEM((T, D), BF),
                pltpu.VMEM((T, HEAD), F32),
                pltpu.VMEM((T, HEAD), F32),
                pltpu.VMEM((SLOTS, D, 2 * W), BF),
                pltpu.VMEM((N, HEADS, T, HEAD), BF),
                pltpu.VMEM((2, N, HEADS, HEAD, T), BF),
                pltpu.VMEM((HEADS, N, T, HEAD), BF),
                pltpu.VMEM((2, HEADS, N, HEAD, T), BF),
                pltpu.VMEM((HEADS, N, T, HEAD), BF),
                pltpu.VMEM((HEADS, N, T, HEAD), BF),
                pltpu.VMEM((T, D), F32),
                pltpu.VMEM((OSLOTS, 2 * HEAD, D), BF),
                pltpu.VMEM((2, 2 * T, T), F32),
                pltpu.VMEM((2, 2 * T, T), F32),
                pltpu.VMEM((CHIPS, 8, T), F32),
                pltpu.VMEM((CHIPS, 2, HEAD + 8, T), F32),
                dma((3,)),
                dma((SLOTS, 4)),
                dma((OSLOTS, 2)),
                dma((3, HEADS, N)),
                dma((3, HEADS, N)),
                dma((HEADS, N)),
                dma((HEADS, N)),
            ],
            compiler_params=pltpu.CompilerParams(collective_id=0, has_side_effects=True, vmem_limit_bytes=52 * 2**20),
        )(*(pltpu.with_memory_space_constraint(t, pltpu.HBM) for t in (x, gain, _table(), wk, wv, wq, wo)))

    tokens, whole = P(("dp", "sp"), None), P(None, None)
    return jax.shard_map(
        step,
        mesh=mesh,
        in_specs=(tokens, P(None), whole, whole, whole, whole),
        out_specs=tokens,
        check_vma=False,
    )
```

```python
import jax
import jax.numpy as jnp
import numpy as np
from jax import lax
from jax.experimental import pallas as pl
from jax.experimental.pallas import tpu as pltpu
from jax.sharding import PartitionSpec as P

HEAD = 128
THETA = 10000
NEG = -1e30
HIDDEN = 2 * NEG
LOG2E = 1.4426950408889634
N = 16
ORDER = ((0, 0), (0, 1), (0, 2), (1, 2), (1, 0), (1, 1))
CHIPS = N // 2
STEPS = CHIPS // 2
T = 256
D = 4096
W = 256
HEADS = W // HEAD
SLOTS = 3
OSLOTS = 4
PIECES = 8
C = D // PIECES
MESH = pl.DeviceIdType.MESH
BF = jnp.bfloat16
F32 = jnp.float32
E = HEAD**-0.5 * LOG2E


def _xor(a, b):
    out = 0
    for bit in (1, 2, 4):
        out = out + bit * lax.rem(lax.div(a, bit) + lax.div(b, bit), 2)
    return out


def _met(chip, i):
    step = lax.div(i, 2)
    even = 1 + step + lax.div(step, 2) - 5 * lax.div(step, 3)
    return _xor(chip, even + lax.rem(i, 2) * (7 - 2 * even))


def _dot(a, b):
    return jnp.dot(a, b, preferred_element_type=F32)


def _kernel(x_ref, gain_ref, table_ref, wk_ref, wv_ref, wq_ref, wo_ref, out_ref,
            x_s, gain_s, table_s, a_s, cos_s, sin_s, w_s, kstage_s, stage_s, k_s, vq_s, ostage_s, o_s, y_s, wo_s, even_s, odd_s, top_s, mix_s,
            x_sem, w_sem, wo_sem, send_sem, recv_sem, osend_sem, orecv_sem):
    me = lax.axis_index("sp")
    chip = lax.div(me, 2)
    i32 = jnp.int32
    weights = (wk_ref, wv_ref, wq_ref)

    def fetch(stage, i, slot):
        h, t = ORDER[stage]
        for n in range(4):
            at = pl.multiple_of((2 * _met(chip, 2 * i + n // 2) + n % 2) * W + h * HEAD, HEAD)
            yield pltpu.make_async_copy(weights[t].at[:, pl.ds(at, HEAD)], w_s.at[slot, :, n * HEAD : (n + 1) * HEAD], w_sem.at[slot, n])

    def start(copies):
        for one in copies:
            one.start()

    def fetch_out(h, i, u, slot):
        at = pl.multiple_of((2 * _met(chip, i) + u) * W + h * HEAD, HEAD)
        return pltpu.make_async_copy(wo_ref.at[pl.ds(at, HEAD), :], wo_s.at[slot, pl.ds(u * HEAD, HEAD)], wo_sem.at[slot, u])

    def copy(t, h, there, place):
        src = kstage_s.at[there, h] if t == 0 else stage_s.at[t - 1, there, h]
        dst = k_s.at[h, place] if t == 0 else vq_s.at[t - 1, h, place]
        return pltpu.make_async_remote_copy(src, dst, send_sem.at[t, h, there], recv_sem.at[t, h, place], device_id={"sp": there}, device_id_type=MESH)

    def copy_out(h, there, place):
        return pltpu.make_async_remote_copy(ostage_s.at[h, there], o_s.at[h, place], osend_sem.at[h, there], orecv_sem.at[h, place],
                                            device_id={"sp": there}, device_id_type=MESH)

    first = [pltpu.make_async_copy(a, b, x_sem.at[n]) for n, (a, b) in enumerate(((x_ref, x_s), (table_ref, table_s), (gain_ref, gain_s)))]
    for one in first:
        one.start()

    barrier = pltpu.get_barrier_semaphore()
    for o in range(1, N):
        pl.semaphore_signal(barrier, inc=1, device_id={"sp": lax.rem(me + o, N)}, device_id_type=MESH)

    start(fetch(0, jnp.int32(0), 0))
    for one in first:
        one.wait()
    for n in range(1, SLOTS):
        start(fetch(0, jnp.int32(n), n))
    gain = gain_s[...].astype(F32).reshape(1, D)

    def norm(r, z):
        rows = pl.ds(pl.multiple_of(r * 32, 32), 32)
        wide = x_s[rows, :].astype(F32)
        scale = lax.rsqrt(jnp.mean(wide * wide, -1, keepdims=True) + 1e-6)
        a_s[rows, :] = (wide * scale * gain).astype(BF)
        return z

    lax.fori_loop(0, T // 32, norm, 0)
    far_cos, far_sin = table_s[0, pl.ds(me, 1), :], table_s[1, pl.ds(me, 1), :]
    near_cos, near_sin = table_s[0, N:, :], table_s[1, N:, :]
    sign = jnp.where(lax.broadcasted_iota(i32, (T, HEAD), 1) < HEAD // 2, -1.0, 1.0).astype(F32)
    cos_s[...] = far_cos * near_cos - far_sin * near_sin
    sin_s[...] = (far_sin * near_cos + far_cos * near_sin) * sign

    def project(stage):
        h, t = ORDER[stage]

        def body(i, z):
            slot = lax.rem(stage * STEPS + i, SLOTS)
            for one in fetch(stage, i, slot):
                one.wait()
            for v in range(2):
                pair = _met(chip, 2 * i + v)
                p = _dot(a_s[...], w_s[slot, :, v * W : (v + 1) * W]).astype(BF)
                for u in range(2):
                    one = p[:, u * HEAD : (u + 1) * HEAD]
                    if t != 1:
                        wide = one.astype(F32)
                        one = (wide * cos_s[...] + pltpu.roll(wide, HEAD // 2, 1) * sin_s[...]).astype(BF)
                    if t == 0:
                        kstage_s[2 * pair + u, h] = one
                    else:
                        stage_s[t - 1, 2 * pair + u, h] = one.T

            @pl.when(i + SLOTS < STEPS)
            def _():
                start(fetch(stage, i + SLOTS, slot))

            if stage < 5:

                @pl.when(i + SLOTS >= STEPS)
                def _():
                    start(fetch(stage + 1, i + SLOTS - STEPS, slot))

            if stage == 0:

                @pl.when(i == 0)
                def _():
                    pl.semaphore_wait(barrier, N - 1)

            for n in range(4):
                there = 2 * _met(chip, 2 * i + n // 2) + n % 2

                if (h, t) != (1, 0):

                    @pl.when(there != me)
                    def _():
                        if (h, t) == (1, 1):
                            copy(0, 1, there, me).start()
                        copy(t, h, there, me).start()

                @pl.when(there == me)
                def _():
                    if t == 0:
                        k_s[h, me] = kstage_s[me, h]
                    else:
                        vq_s[t - 1, h, me] = stage_s[t - 1, me, h]

            return z

        lax.fori_loop(0, STEPS, body, 0)

    def others(i, do):
        for u in range(2):
            there = 2 * _met(chip, i) + u

            @pl.when(there != me)
            def _():
                do(there)

    def each(do):
        def body(i, z):
            others(i, do)
            return z

        lax.fori_loop(0, CHIPS, body, 0)

    project(0)
    project(1)
    project(2)
    project(3)
    project(4)
    project(5)
    for n in range(OSLOTS):
        for u in range(2):
            fetch_out(0, jnp.int32(n), u, n).start()
    y_s[...] = x_s[...].astype(F32)

    def output(h, i, last):
        pair = _met(chip, i)
        slot = lax.rem(i, OSLOTS)
        for u in range(2):
            there = 2 * pair + u

            @pl.when(there != me)
            def _():
                copy_out(h, there, there).wait_recv()

            fetch_out(h, i, u, slot).wait()
        o = jnp.concatenate([o_s[h, 2 * pair], o_s[h, 2 * pair + 1]], axis=1)
        for c in range(PIECES):
            cols = slice(c * C, (c + 1) * C)
            y = y_s[:, cols] + _dot(o, wo_s[slot, :, cols])
            if last:
                out_ref[:, cols] = y.astype(BF)
            else:
                y_s[:, cols] = y

        if not last:

            @pl.when(i + OSLOTS < CHIPS)
            def _():
                for u in range(2):
                    fetch_out(h, i + OSLOTS, u, slot).start()

            if h == 0:

                @pl.when(i + OSLOTS >= CHIPS)
                def _():
                    for u in range(2):
                        fetch_out(1, i + OSLOTS - CHIPS, u, slot).start()

    ones = jnp.ones((8, T), BF)

    def score(h, pair, j, buf):
        k = k_s[h, pl.ds(2 * j, 2)].reshape(2 * T, HEAD)
        for u in range(2):
            buf[u] = _dot(k, vq_s[1, h, 2 * pair + u])

    def take(h, pair, j, buf, masked):
        for u in range(2):
            parts = u + 1 if masked else 2
            s = buf[u, : parts * T]
            if masked:
                gap = lax.broadcasted_iota(i32, s.shape, 1) - lax.broadcasted_iota(i32, s.shape, 0)
                s = jnp.where(gap >= -u * T, s, HIDDEN)
            old = top_s[pair, u : u + 1, :]
            top = jnp.maximum(old, s.max(axis=0, keepdims=True))
            top_s[pair, u : u + 1, :] = top
            p = jnp.exp2((s - top) * E).astype(BF)
            keep = jnp.exp2((old - top) * E)
            mix = mix_s[pair, u] * keep
            for n in range(parts):
                v = jnp.concatenate([vq_s[0, h, 2 * j + n], ones], axis=0)
                mix += _dot(v, p[n * T : (n + 1) * T, :])
            mix_s[pair, u] = mix

    def clear():
        top_s[...] = jnp.full(top_s.shape, NEG, F32)

        def body(pair, z):
            mix_s[pair] = jnp.zeros(mix_s.shape[1:], F32)
            return z

        lax.fori_loop(0, CHIPS, body, 0)

    def finish(h, pair):
        for u in range(2):
            o = (mix_s[pair, u, :HEAD, :] * (1 / mix_s[pair, u, HEAD : HEAD + 1, :])).astype(BF).T
            ostage_s[h, 2 * pair + u] = o

        for u in range(2):
            there = 2 * pair + u

            @pl.when(there == me)
            def _():
                o_s[h, me] = ostage_s[h, me]

            @pl.when(there != me)
            def _():
                copy_out(h, there, me).start()

    def await_all(h, t):
        each(lambda there: copy(t, h, there, there).wait_recv())

    def by_queries(i, z):
        pair = _met(chip, i)
        others(i, lambda there: copy(2, 0, there, there).wait_recv())

        def two(n, z):
            j = 2 * n
            score(0, pair, j + 1, odd_s)
            take(0, pair, j, even_s, False)
            score(0, pair, j + 2, even_s)
            take(0, pair, j + 1, odd_s, False)
            return z

        score(0, pair, 0, even_s)
        lax.fori_loop(0, lax.div(pair, 2), two, 0)

        @pl.when(lax.rem(pair, 2) == 0)
        def _():
            take(0, pair, pair, even_s, True)

        @pl.when(lax.rem(pair, 2) == 1)
        def _():
            score(0, pair, pair, odd_s)
            take(0, pair, pair - 1, even_s, False)
            take(0, pair, pair, odd_s, True)

        finish(0, pair)
        return z

    def by_keys(i, z):
        j = _met(chip, i)

        def await_pair(there):
            copy(0, 1, there, there).wait_recv()
            copy(1, 1, there, there).wait_recv()

        others(i, await_pair)
        score(1, j, j, even_s)
        score(1, jnp.minimum(j + 1, CHIPS - 1), j, odd_s)
        take(1, j, j, even_s, True)

        def two(n, z):
            pair = j + 1 + 2 * n
            score(1, pair + 1, j, even_s)
            take(1, pair, j, odd_s, False)
            score(1, jnp.minimum(pair + 2, CHIPS - 1), j, odd_s)
            take(1, pair + 1, j, even_s, False)
            return z

        rest = CHIPS - 1 - j
        lax.fori_loop(0, lax.div(rest, 2), two, 0)

        @pl.when(lax.rem(rest, 2) == 1)
        def _():
            take(1, CHIPS - 1, j, odd_s, False)

        return z

    def finish_step(i, z):
        finish(1, _met(chip, i))
        return z

    clear()
    await_all(0, 0)
    await_all(0, 1)
    lax.fori_loop(0, CHIPS, by_queries, 0)
    clear()
    await_all(1, 2)
    lax.fori_loop(0, CHIPS, by_keys, 0)
    lax.fori_loop(0, CHIPS, finish_step, 0)

    for h in range(HEADS):

        def output_step(i, z):
            output(h, i, False)
            return z

        lax.fori_loop(0, CHIPS - h, output_step, 0)

    def drain(there):
        for h in range(HEADS):
            for t in range(3):
                copy(t, h, there, me).wait_send()
        copy_out(0, there, me).wait_send()

    each(drain)
    output(1, jnp.int32(CHIPS - 1), True)
    each(lambda there: copy_out(1, there, me).wait_send())


def _table():
    half = HEAD // 2
    rate = THETA ** (-(np.arange(HEAD) % half).astype(np.float64) / half)
    angle = np.concatenate([np.arange(N) * T, np.arange(T)])[:, None] * rate
    return jnp.asarray(np.stack([np.cos(angle), np.sin(angle)]), F32)


def solution(mesh):
    def step(x, gain, wq, wk, wv, wo):
        dma = pltpu.SemaphoreType.DMA
        return pl.pallas_call(
            _kernel,
            out_shape=pltpu.VMEM((T, D), BF),
            in_specs=[pl.BlockSpec(memory_space=pltpu.HBM)] * 7,
            out_specs=pl.BlockSpec(memory_space=pltpu.VMEM),
            scratch_shapes=[
                pltpu.VMEM((T, D), BF),
                pltpu.VMEM((D,), BF),
                pltpu.VMEM((2, N + T, HEAD), F32),
                pltpu.VMEM((T, D), BF),
                pltpu.VMEM((T, HEAD), F32),
                pltpu.VMEM((T, HEAD), F32),
                pltpu.VMEM((SLOTS, D, 2 * W), BF),
                pltpu.VMEM((N, HEADS, T, HEAD), BF),
                pltpu.VMEM((2, N, HEADS, HEAD, T), BF),
                pltpu.VMEM((HEADS, N, T, HEAD), BF),
                pltpu.VMEM((2, HEADS, N, HEAD, T), BF),
                pltpu.VMEM((HEADS, N, T, HEAD), BF),
                pltpu.VMEM((HEADS, N, T, HEAD), BF),
                pltpu.VMEM((T, D), F32),
                pltpu.VMEM((OSLOTS, 2 * HEAD, D), BF),
                pltpu.VMEM((2, 2 * T, T), F32),
                pltpu.VMEM((2, 2 * T, T), F32),
                pltpu.VMEM((CHIPS, 8, T), F32),
                pltpu.VMEM((CHIPS, 2, HEAD + 8, T), F32),
                dma((3,)),
                dma((SLOTS, 4)),
                dma((OSLOTS, 2)),
                dma((3, HEADS, N)),
                dma((3, HEADS, N)),
                dma((HEADS, N)),
                dma((HEADS, N)),
            ],
            compiler_params=pltpu.CompilerParams(collective_id=0, has_side_effects=True, vmem_limit_bytes=52 * 2**20),
        )(*(pltpu.with_memory_space_constraint(t, pltpu.HBM) for t in (x, gain, _table(), wk, wv, wq, wo)))

    tokens, whole = P(("dp", "sp"), None), P(None, None)
    return jax.shard_map(
        step,
        mesh=mesh,
        in_specs=(tokens, P(None), whole, whole, whole, whole),
        out_specs=tokens,
        check_vma=False,
    )
```

```python
import jax
import jax.numpy as jnp
import numpy as np
from jax import lax
from jax.experimental import pallas as pl
from jax.experimental.pallas import tpu as pltpu
from jax.sharding import PartitionSpec as P

HEAD = 128
THETA = 10000
NEG = -1e30
HIDDEN = 2 * NEG
LOG2E = 1.4426950408889634
N = 16
ORDER = ((0, 0), (0, 1), (0, 2), (1, 2), (1, 0), (1, 1))
CHIPS = N // 2
STEPS = CHIPS // 2
T = 256
D = 4096
W = 256
HEADS = W // HEAD
SLOTS = 3
OSLOTS = 4
PIECES = 8
C = D // PIECES
MESH = pl.DeviceIdType.MESH
BF = jnp.bfloat16
F32 = jnp.float32
E = HEAD**-0.5 * LOG2E


def _xor(a, b):
    out = 0
    for bit in (1, 2, 4):
        out = out + bit * lax.rem(lax.div(a, bit) + lax.div(b, bit), 2)
    return out


def _met(chip, i):
    step = lax.div(i, 2)
    even = 1 + step + lax.div(step, 2) - 5 * lax.div(step, 3)
    return _xor(chip, even + lax.rem(i, 2) * (7 - 2 * even))


def _dot(a, b):
    return jnp.dot(a, b, preferred_element_type=F32)


def _kernel(x_ref, gain_ref, table_ref, wk_ref, wv_ref, wq_ref, wo_ref, out_ref,
            x_s, gain_s, table_s, a_s, cos_s, sin_s, w_s, kstage_s, stage_s, k_s, vq_s, ostage_s, o_s, y_s, wo_s, even_s, odd_s, top_s, mix_s,
            x_sem, w_sem, wo_sem, send_sem, recv_sem, osend_sem, orecv_sem):
    me = lax.axis_index("sp")
    chip = lax.div(me, 2)
    i32 = jnp.int32
    weights = (wk_ref, wv_ref, wq_ref)

    def fetch(stage, i, slot):
        h, t = ORDER[stage]
        for n in range(4):
            at = pl.multiple_of((2 * _met(chip, 2 * i + n // 2) + n % 2) * W + h * HEAD, HEAD)
            yield pltpu.make_async_copy(weights[t].at[:, pl.ds(at, HEAD)], w_s.at[slot, :, n * HEAD : (n + 1) * HEAD], w_sem.at[slot, n])

    def start(copies):
        for one in copies:
            one.start()

    def fetch_out(h, i, u, slot):
        at = pl.multiple_of((2 * _met(chip, i) + u) * W + h * HEAD, HEAD)
        return pltpu.make_async_copy(wo_ref.at[pl.ds(at, HEAD), :], wo_s.at[slot, pl.ds(u * HEAD, HEAD)], wo_sem.at[slot, u])

    def copy(t, h, there, place):
        src = kstage_s.at[there, h] if t == 0 else stage_s.at[t - 1, there, h]
        dst = k_s.at[h, place] if t == 0 else vq_s.at[t - 1, h, place]
        return pltpu.make_async_remote_copy(src, dst, send_sem.at[t, h, there], recv_sem.at[t, h, place], device_id={"sp": there}, device_id_type=MESH)

    def copy_out(h, there, place):
        return pltpu.make_async_remote_copy(ostage_s.at[h, there], o_s.at[h, place], osend_sem.at[h, there], orecv_sem.at[h, place],
                                            device_id={"sp": there}, device_id_type=MESH)

    first = [pltpu.make_async_copy(a, b, x_sem.at[n]) for n, (a, b) in enumerate(((x_ref, x_s), (table_ref, table_s), (gain_ref, gain_s)))]
    for one in first:
        one.start()

    barrier = pltpu.get_barrier_semaphore()
    for o in range(1, N):
        pl.semaphore_signal(barrier, inc=1, device_id={"sp": lax.rem(me + o, N)}, device_id_type=MESH)

    start(fetch(0, jnp.int32(0), 0))
    start(fetch(0, jnp.int32(1), 1))
    for one in first:
        one.wait()
    for n in range(2, SLOTS):
        start(fetch(0, jnp.int32(n), n))
    gain = gain_s[...].astype(F32).reshape(1, D)

    def norm(r, z):
        rows = pl.ds(pl.multiple_of(r * 32, 32), 32)
        wide = x_s[rows, :].astype(F32)
        scale = lax.rsqrt(jnp.mean(wide * wide, -1, keepdims=True) + 1e-6)
        a_s[rows, :] = (wide * scale * gain).astype(BF)
        return z

    lax.fori_loop(0, T // 32, norm, 0)
    far_cos, far_sin = table_s[0, pl.ds(me, 1), :], table_s[1, pl.ds(me, 1), :]
    near_cos, near_sin = table_s[0, N:, :], table_s[1, N:, :]
    sign = jnp.where(lax.broadcasted_iota(i32, (T, HEAD), 1) < HEAD // 2, -1.0, 1.0).astype(F32)
    cos_s[...] = far_cos * near_cos - far_sin * near_sin
    sin_s[...] = (far_sin * near_cos + far_cos * near_sin) * sign

    def project(stage):
        h, t = ORDER[stage]

        def body(i, z):
            slot = lax.rem(stage * STEPS + i, SLOTS)
            for one in fetch(stage, i, slot):
                one.wait()
            for v in range(2):
                pair = _met(chip, 2 * i + v)
                p = _dot(a_s[...], w_s[slot, :, v * W : (v + 1) * W]).astype(BF)
                for u in range(2):
                    one = p[:, u * HEAD : (u + 1) * HEAD]
                    if t != 1:
                        wide = one.astype(F32)
                        one = (wide * cos_s[...] + pltpu.roll(wide, HEAD // 2, 1) * sin_s[...]).astype(BF)
                    if t == 0:
                        kstage_s[2 * pair + u, h] = one
                    else:
                        stage_s[t - 1, 2 * pair + u, h] = one.T

            @pl.when(i + SLOTS < STEPS)
            def _():
                start(fetch(stage, i + SLOTS, slot))

            if stage < 5:

                @pl.when(i + SLOTS >= STEPS)
                def _():
                    start(fetch(stage + 1, i + SLOTS - STEPS, slot))

            if stage == 0:

                @pl.when(i == 0)
                def _():
                    pl.semaphore_wait(barrier, N - 1)

            for n in range(4):
                there = 2 * _met(chip, 2 * i + n // 2) + n % 2

                if (h, t) != (1, 0):

                    @pl.when(there != me)
                    def _():
                        if (h, t) == (1, 1):
                            copy(0, 1, there, me).start()
                        copy(t, h, there, me).start()

                @pl.when(there == me)
                def _():
                    if t == 0:
                        k_s[h, me] = kstage_s[me, h]
                    else:
                        vq_s[t - 1, h, me] = stage_s[t - 1, me, h]

            return z

        lax.fori_loop(0, STEPS, body, 0)

    def others(i, do):
        for u in range(2):
            there = 2 * _met(chip, i) + u

            @pl.when(there != me)
            def _():
                do(there)

    def each(do):
        def body(i, z):
            others(i, do)
            return z

        lax.fori_loop(0, CHIPS, body, 0)

    project(0)
    project(1)
    project(2)
    project(3)
    project(4)
    project(5)
    for n in range(OSLOTS):
        for u in range(2):
            fetch_out(0, jnp.int32(n), u, n).start()
    y_s[...] = x_s[...].astype(F32)

    def output(h, i, last):
        pair = _met(chip, i)
        slot = lax.rem(i, OSLOTS)
        for u in range(2):
            there = 2 * pair + u

            @pl.when(there != me)
            def _():
                copy_out(h, there, there).wait_recv()

            fetch_out(h, i, u, slot).wait()
        o = jnp.concatenate([o_s[h, 2 * pair], o_s[h, 2 * pair + 1]], axis=1)
        for c in range(PIECES):
            cols = slice(c * C, (c + 1) * C)
            y = y_s[:, cols] + _dot(o, wo_s[slot, :, cols])
            if last:
                out_ref[:, cols] = y.astype(BF)
            else:
                y_s[:, cols] = y

        if not last:

            @pl.when(i + OSLOTS < CHIPS)
            def _():
                for u in range(2):
                    fetch_out(h, i + OSLOTS, u, slot).start()

            if h == 0:

                @pl.when(i + OSLOTS >= CHIPS)
                def _():
                    for u in range(2):
                        fetch_out(1, i + OSLOTS - CHIPS, u, slot).start()

    ones = jnp.ones((8, T), BF)

    def score(h, pair, j, buf):
        k = k_s[h, pl.ds(2 * j, 2)].reshape(2 * T, HEAD)
        for u in range(2):
            buf[u] = _dot(k, vq_s[1, h, 2 * pair + u])

    def take(h, pair, j, buf, masked):
        for u in range(2):
            parts = u + 1 if masked else 2
            s = buf[u, : parts * T]
            if masked:
                gap = lax.broadcasted_iota(i32, s.shape, 1) - lax.broadcasted_iota(i32, s.shape, 0)
                s = jnp.where(gap >= -u * T, s, HIDDEN)
            old = top_s[pair, u : u + 1, :]
            top = jnp.maximum(old, s.max(axis=0, keepdims=True))
            top_s[pair, u : u + 1, :] = top
            p = jnp.exp2((s - top) * E).astype(BF)
            keep = jnp.exp2((old - top) * E)
            mix = mix_s[pair, u] * keep
            for n in range(parts):
                v = jnp.concatenate([vq_s[0, h, 2 * j + n], ones], axis=0)
                mix += _dot(v, p[n * T : (n + 1) * T, :])
            mix_s[pair, u] = mix

    def clear():
        top_s[...] = jnp.full(top_s.shape, NEG, F32)

        def body(pair, z):
            mix_s[pair] = jnp.zeros(mix_s.shape[1:], F32)
            return z

        lax.fori_loop(0, CHIPS, body, 0)

    def finish(h, pair):
        for u in range(2):
            o = (mix_s[pair, u, :HEAD, :] * (1 / mix_s[pair, u, HEAD : HEAD + 1, :])).astype(BF).T
            ostage_s[h, 2 * pair + u] = o

        for u in range(2):
            there = 2 * pair + u

            @pl.when(there == me)
            def _():
                o_s[h, me] = ostage_s[h, me]

            @pl.when(there != me)
            def _():
                copy_out(h, there, me).start()

    def await_all(h, t):
        each(lambda there: copy(t, h, there, there).wait_recv())

    def by_queries(i, z):
        pair = _met(chip, i)
        others(i, lambda there: copy(2, 0, there, there).wait_recv())

        def two(n, z):
            j = 2 * n
            score(0, pair, j + 1, odd_s)
            take(0, pair, j, even_s, False)
            score(0, pair, j + 2, even_s)
            take(0, pair, j + 1, odd_s, False)
            return z

        score(0, pair, 0, even_s)
        lax.fori_loop(0, lax.div(pair, 2), two, 0)

        @pl.when(lax.rem(pair, 2) == 0)
        def _():
            take(0, pair, pair, even_s, True)

        @pl.when(lax.rem(pair, 2) == 1)
        def _():
            score(0, pair, pair, odd_s)
            take(0, pair, pair - 1, even_s, False)
            take(0, pair, pair, odd_s, True)

        finish(0, pair)
        return z

    def by_keys(i, z):
        j = _met(chip, i)

        def await_pair(there):
            copy(0, 1, there, there).wait_recv()
            copy(1, 1, there, there).wait_recv()

        others(i, await_pair)
        score(1, j, j, even_s)
        score(1, jnp.minimum(j + 1, CHIPS - 1), j, odd_s)
        take(1, j, j, even_s, True)

        def two(n, z):
            pair = j + 1 + 2 * n
            score(1, pair + 1, j, even_s)
            take(1, pair, j, odd_s, False)
            score(1, jnp.minimum(pair + 2, CHIPS - 1), j, odd_s)
            take(1, pair + 1, j, even_s, False)
            return z

        rest = CHIPS - 1 - j
        lax.fori_loop(0, lax.div(rest, 2), two, 0)

        @pl.when(lax.rem(rest, 2) == 1)
        def _():
            take(1, CHIPS - 1, j, odd_s, False)

        return z

    def finish_step(i, z):
        finish(1, _met(chip, i))
        return z

    clear()
    await_all(0, 0)
    await_all(0, 1)
    lax.fori_loop(0, CHIPS, by_queries, 0)
    clear()
    await_all(1, 2)
    lax.fori_loop(0, CHIPS, by_keys, 0)
    lax.fori_loop(0, CHIPS, finish_step, 0)

    for h in range(HEADS):

        def output_step(i, z):
            output(h, i, False)
            return z

        lax.fori_loop(0, CHIPS - h, output_step, 0)

    def drain(there):
        for h in range(HEADS):
            for t in range(3):
                copy(t, h, there, me).wait_send()
        copy_out(0, there, me).wait_send()

    each(drain)
    output(1, jnp.int32(CHIPS - 1), True)
    each(lambda there: copy_out(1, there, me).wait_send())


def _table():
    half = HEAD // 2
    rate = THETA ** (-(np.arange(HEAD) % half).astype(np.float64) / half)
    angle = np.concatenate([np.arange(N) * T, np.arange(T)])[:, None] * rate
    return jnp.asarray(np.stack([np.cos(angle), np.sin(angle)]), F32)


def solution(mesh):
    def step(x, gain, wq, wk, wv, wo):
        dma = pltpu.SemaphoreType.DMA
        return pl.pallas_call(
            _kernel,
            out_shape=pltpu.VMEM((T, D), BF),
            in_specs=[pl.BlockSpec(memory_space=pltpu.HBM)] * 7,
            out_specs=pl.BlockSpec(memory_space=pltpu.VMEM),
            scratch_shapes=[
                pltpu.VMEM((T, D), BF),
                pltpu.VMEM((D,), BF),
                pltpu.VMEM((2, N + T, HEAD), F32),
                pltpu.VMEM((T, D), BF),
                pltpu.VMEM((T, HEAD), F32),
                pltpu.VMEM((T, HEAD), F32),
                pltpu.VMEM((SLOTS, D, 2 * W), BF),
                pltpu.VMEM((N, HEADS, T, HEAD), BF),
                pltpu.VMEM((2, N, HEADS, HEAD, T), BF),
                pltpu.VMEM((HEADS, N, T, HEAD), BF),
                pltpu.VMEM((2, HEADS, N, HEAD, T), BF),
                pltpu.VMEM((HEADS, N, T, HEAD), BF),
                pltpu.VMEM((HEADS, N, T, HEAD), BF),
                pltpu.VMEM((T, D), F32),
                pltpu.VMEM((OSLOTS, 2 * HEAD, D), BF),
                pltpu.VMEM((2, 2 * T, T), F32),
                pltpu.VMEM((2, 2 * T, T), F32),
                pltpu.VMEM((CHIPS, 8, T), F32),
                pltpu.VMEM((CHIPS, 2, HEAD + 8, T), F32),
                dma((3,)),
                dma((SLOTS, 4)),
                dma((OSLOTS, 2)),
                dma((3, HEADS, N)),
                dma((3, HEADS, N)),
                dma((HEADS, N)),
                dma((HEADS, N)),
            ],
            compiler_params=pltpu.CompilerParams(collective_id=0, has_side_effects=True, vmem_limit_bytes=52 * 2**20),
        )(*(pltpu.with_memory_space_constraint(t, pltpu.HBM) for t in (x, gain, _table(), wk, wv, wq, wo)))

    tokens, whole = P(("dp", "sp"), None), P(None, None)
    return jax.shard_map(
        step,
        mesh=mesh,
        in_specs=(tokens, P(None), whole, whole, whole, whole),
        out_specs=tokens,
        check_vma=False,
    )
```
